32 devices in a mesh: area: 8 (over y, x, core), rank: 4 (over z).
Axes of the slice: x: 2, y: 2, z: 4, core: 2. Of those that a mesh axis runs over, the one named last changes fastest.
Arguments:
- initial_bits: int32 [2, 48, 128], P(None, None, ('area', 'rank')), may hold values from -2147483648 to 2147483646
- membrane: float32 [48, 4096], P(None, ('area', 'rank')), may hold values from -100 to 200
- drive: int32 [4096], P(('area', 'rank')), may hold values from 0 to 47
- leak_shift: int32 [4096], P(('area', 'rank')), may hold values from 2 to 5
- weights: bfloat16 [32, 128, 128, 128], P(('area', 'rank')), may hold values from -3 to 3, as said below
- pre_block: int32 [32, 128], P(('area', 'rank')), may hold values from 0 to 31
- block_mask: int32 [32, 128], P(('area', 'rank')), may hold values 0 or 1
- delay: int32 [32, 128], P(('area', 'rank')), may hold values from 2 to 5
- area_of_block: int32 [32, 1], replicated, may hold values from 0 to 31
Outputs:
- final_membrane: float32 [48, 4096], P(None, ('area', 'rank'))
- area_rates: float32 [10, 32], replicated
The draws below stay inside these ranges and needn't reach their ends.
Inputs may be any that keep to these rules, and one draw needn't show every extreme that they name: weights hold whole numbers. `area_of_block`: every area holds at least one block.
All inputs are finite; a program needn't handle non-finite values. No bound on the sum of `block_mask` on one device may be relied on, other than what follows from the above.
Results may differ from the reference program's by a relative error of at most 0.0003.
Values sent between devices are 32-bit elements; how exact they have to be, the bound alone decides.
A program may use at most 128 MiB of HBM per device.

```python
import jax
import jax.numpy as jnp
from jax import lax

BLOCK = 128
AREAS = 32
K = 128
TRIALS = 48
DMIN = 2
NDELAY = 4
STEPS = 10
BLOCKS = 32
NEURONS = 4096


def draw_weights(key, part):
    values = jax.random.randint(key, (BLOCKS, K, BLOCK, BLOCK), -3, 4)
    return values.astype(jnp.float32).astype(jnp.bfloat16)


def with_ends(result, stream_key, smallest, top_value):
    extent = result.shape
    index_at = [jax.random.randint(jax.random.fold_in(stream_key, axis), (), 0, extent[axis]) for axis in range(len(extent))]
    result = result.at[tuple(index_at)].set(smallest)
    longest = extent.index(max(extent))
    index_at[longest] = (index_at[longest] + 1) % extent[longest]
    return result.at[tuple(index_at)].set(top_value)


def block_levels(stream_key, shape, shards, smallest, largest):
    def one(position, shards_of):
        draws = jax.random.uniform(jax.random.fold_in(jax.random.fold_in(stream_key, 6), position), (shards_of,), jnp.float32, smallest / len(shards), largest / len(shards))
        return jnp.repeat(jnp.exp(draws), shape[position] // shards_of).reshape((-1,) + (1,) * (len(shape) - position - 1))

    gain = one(*shards[0])
    for cut in shards[1:]:
        gain = gain * one(*cut)
    return gain


def different_ones(own_key, rows, amount, top, lift):
    ranking = jax.random.permutation(jax.random.fold_in(own_key, 1), amount)
    favour = ranking
    for power in range(3):
        favour = favour * favour // amount
    favour = favour * lift // amount
    tickets = jax.random.randint(jax.random.fold_in(own_key, 2), (rows, amount), 0, 4096) + favour
    sure = jax.random.permutation(jax.random.fold_in(own_key, 3), rows)[jnp.arange(amount) % rows]
    tickets = jnp.where(jnp.arange(rows)[:, None] == sure[None, :], 1 << 14, tickets)
    merit = tickets * amount + jnp.arange(amount)
    return lax.top_k(merit.astype(jnp.int32), top)[1].astype(jnp.int32)


def setup_inputs(seed: int = 0) -> dict:
    arg_keys = jax.random.split(jax.random.key(seed), 10)
    initial_bits = with_ends(jax.random.randint(arg_keys[0], (DMIN, TRIALS, NEURONS // 32), -2147483648, 2147483647), jax.random.fold_in(arg_keys[0], 1), -2147483648, 2147483646).astype(jnp.int32)
    membrane = jnp.clip(-100.0 + 300.0 * jax.random.uniform(arg_keys[1], (TRIALS, NEURONS), jnp.float32) ** block_levels(arg_keys[1], (TRIALS, NEURONS), ((1, 32),), -0.2, 0.2), -100.0, 200.0)
    drive = with_ends(jax.random.randint(arg_keys[2], (NEURONS,), 0, 48), jax.random.fold_in(arg_keys[2], 1), 0, 47).astype(jnp.int32)
    leak_shift = with_ends(jax.random.randint(arg_keys[3], (NEURONS,), 2, 6), jax.random.fold_in(arg_keys[3], 1), 2, 5).astype(jnp.int32)
    weights = draw_weights(jax.random.fold_in(arg_keys[9], 71), 0)
    pre_block = with_ends(jax.random.randint(arg_keys[5], (BLOCKS, K), 0, BLOCKS), jax.random.fold_in(arg_keys[5], 1), 0, BLOCKS - 1).astype(jnp.int32)
    block_mask = with_ends((jax.random.randint(arg_keys[6], (BLOCKS, K), 0, 4) < 3).astype(jnp.int32), jax.random.fold_in(arg_keys[6], 1), 0, 1)
    delay = with_ends(jax.random.randint(arg_keys[7], (BLOCKS, K), DMIN, DMIN + NDELAY), jax.random.fold_in(arg_keys[7], 1), DMIN, (DMIN + NDELAY) - 1).astype(jnp.int32)
    area_of_block = different_ones(arg_keys[8], BLOCKS, AREAS, 1, 512)
    return dict(initial_bits=initial_bits, membrane=membrane, drive=drive, leak_shift=leak_shift, weights=weights, pre_block=pre_block, block_mask=block_mask, delay=delay, area_of_block=area_of_block)


threshold_level = 200.0


def unpack(packed):
    shifts = jnp.arange(32, dtype=jnp.int32)
    bit_values = jnp.bitwise_and(jnp.right_shift(packed[..., None], shifts), 1)
    return bit_values.reshape(packed.shape[:-1] + (packed.shape[-1] * 32,))


def reference(initial_bits, membrane, drive, leak_shift, weights, pre_block, block_mask, delay, area_of_block):
    neurons = BLOCKS * BLOCK
    intervals = STEPS // DMIN
    lag_table = (delay[:, :, None] - DMIN == jnp.arange(NDELAY, dtype=jnp.int32)[None, None, :]).astype(jnp.float32)
    input_weighting = block_mask.astype(jnp.float32)[:, :, None] * lag_table
    buffer = jnp.zeros((STEPS + NDELAY, TRIALS, neurons), jnp.float32)
    history = unpack(initial_bits).astype(jnp.float32)
    membrane_voltage = jnp.floor(membrane)
    leak_scale = 1.0 / jnp.left_shift(jnp.ones_like(leak_shift), leak_shift).astype(jnp.float32)
    drive_float = drive.astype(jnp.float32)
    area_table = (area_of_block[:, 0:1] == jnp.arange(AREAS, dtype=jnp.int32)[None, :]).astype(jnp.float32)
    block_counts = []
    for interval in range(intervals):
        source_rows = history.reshape(DMIN * TRIALS, BLOCKS, BLOCK)

        def one_block(operands):
            synapses, source, delay_weight_table = operands
            selected = jnp.take(source_rows, source, axis=1).astype(jnp.float32)
            product = jnp.einsum("rkm,kmn->krn", selected, synapses.astype(jnp.float32), precision=lax.Precision.HIGHEST)
            return jnp.einsum("kd,krn->drn", delay_weight_table, product, precision=lax.Precision.HIGHEST)

        arrived = lax.map(one_block, (weights, pre_block, input_weighting))
        arrived = arrived.reshape(BLOCKS, NDELAY, DMIN, TRIALS, BLOCK)
        arrived = jnp.transpose(arrived, (1, 2, 3, 0, 4)).reshape(NDELAY, DMIN, TRIALS, neurons)
        first_step = (interval - 1) * DMIN
        for lag_index in range(NDELAY):
            for offset in range(DMIN):
                landing = first_step + offset + DMIN + lag_index
                buffer = buffer.at[landing].add(arrived[lag_index, offset])
        fired_list = []
        for offset in range(DMIN):
            current = buffer[interval * DMIN + offset]
            membrane_voltage = membrane_voltage - jnp.floor(membrane_voltage * leak_scale) + current + drive_float
            current_spike_flags = membrane_voltage >= threshold_level
            membrane_voltage = jnp.where(current_spike_flags, jnp.zeros_like(membrane_voltage), jnp.maximum(membrane_voltage, -threshold_level))
            spikes = current_spike_flags.astype(jnp.float32)
            fired_list.append(spikes)
            block_counts.append(jnp.sum(spikes.reshape(TRIALS, BLOCKS, BLOCK), axis=(0, 2)))
        history = jnp.stack(fired_list)
    counts = jnp.dot(jnp.stack(block_counts), area_table, precision=lax.Precision.HIGHEST)
    sizes_per_area = jnp.sum(area_table, axis=0) * (TRIALS * BLOCK)
    return membrane_voltage, counts / sizes_per_area
```

```python
import functools

import jax
import jax.numpy as jnp
from jax import lax
from jax.experimental import pallas as pl
from jax.experimental.pallas import tpu as pltpu
from jax.sharding import PartitionSpec as P

AREAS = 32
DMIN = 2
NDELAY = 4
STEPS = 10
DMAX = DMIN + NDELAY - 1
INTERVALS = STEPS // DMIN
SPAN = STEPS + DMAX - DMIN
THRESHOLD = 200.0
GROUP = 8
MESH = pl.DeviceIdType.MESH


def pack(spikes):
    rows = spikes.shape[0] // 8
    word = spikes[0:8]
    for j in range(1, rows):
        word = word | (spikes[8 * j : 8 * j + 8] << j)
    return word[0:4] | (word[4:8] << rows)


def unpack(word, rows):
    word = jnp.concatenate([word, word >> rows], axis=0)
    parts = [(word & (1 << j)) != 0 for j in range(rows)]
    parts = [jnp.where(p, 1.0, 0.0) for p in parts]
    return jnp.concatenate(parts, axis=0).astype(jnp.bfloat16)


def kernel(
    sizes,
    pre_ref,
    mask_ref,
    delay_ref,
    area_ref,
    bits_ref,
    membrane_ref,
    drive_ref,
    leak_ref,
    weights_hbm,
    voltage_ref,
    rates_ref,
    weights_ref,
    history,
    outbox,
    inbox,
    count_out,
    count_in,
    base_ref,
    stride_ref,
    weight_sem,
    send_sem,
    recv_sem,
):
    areas_axis, ranks = sizes
    n = areas_axis * ranks
    me = lax.axis_index("area") * ranks + lax.axis_index("rank")
    trials, block = membrane_ref.shape
    slots = pre_ref.shape[1]
    pair = DMIN * trials
    rows = pair // 8

    load = pltpu.make_async_copy(weights_hbm, weights_ref, weight_sem)
    load.start()

    def coords(j):
        other = lax.rem(me + j, n)
        return (other // ranks, lax.rem(other, ranks))

    barrier = pltpu.get_barrier_semaphore()

    @pl.loop(1, n)
    def _(j):
        pl.semaphore_signal(barrier, inc=1, device_id=coords(j), device_id_type=MESH)

    lane = lax.broadcasted_iota(jnp.int32, (trials, block), 1)
    start = []
    for offset in range(DMIN):
        words = bits_ref[offset]
        spread = jnp.broadcast_to(words[:, 0:1], (trials, block))
        for w in range(1, block // 32):
            spread = jnp.where(lane // 32 == w, words[:, w : w + 1], spread)
        start.append((spread >> (lane % 32)) & 1)
    word = pack(jnp.concatenate(start, axis=0))

    def send(interval, word):
        outbox[interval] = word
        inbox[interval, me] = word

        @pl.loop(1, n)
        def _(j):
            pltpu.make_async_remote_copy(
                src_ref=outbox.at[interval],
                dst_ref=inbox.at[interval, me],
                send_sem=send_sem.at[interval],
                recv_sem=recv_sem.at[interval],
                device_id=coords(j),
                device_id_type=MESH,
            ).start()

    def wait(box, sem):
        region = box.at[pl.ds(0, n - 1)]
        pltpu.make_async_copy(region, region, sem).wait()

    pl.semaphore_wait(barrier, n - 1)
    send(0, word)

    @pl.loop(0, slots)
    def _(k):
        on = mask_ref[0, k]
        base_ref[k] = on * (pre_ref[0, k] * SPAN + (DMAX - delay_ref[0, k]))
        stride_ref[k] = on * DMIN

    early = DMAX - DMIN
    blank = jnp.zeros((trials, block), jnp.bfloat16)

    @pl.loop(0, n)
    def _(b):
        for s in range(early):
            history[b * SPAN + s] = blank

    scale = 1.0 / jnp.left_shift(jnp.ones_like(leak_ref[...]), leak_ref[...]).astype(jnp.float32)
    push = drive_ref[...].astype(jnp.float32)
    voltage = jnp.floor(membrane_ref[...])
    count_lane = lax.broadcasted_iota(jnp.int32, (1, block), 1)
    counts = jnp.zeros((1, block), jnp.float32)
    area_row = lax.broadcasted_iota(jnp.int32, (AREAS, block), 0)

    def tally(b, total):
        return total + jnp.where(area_row == area_ref[0, b], 1.0, 0.0)

    members = lax.fori_loop(0, n, tally, jnp.zeros((AREAS, block), jnp.float32))

    for interval in range(INTERVALS):
        wait(inbox.at[interval], recv_sem.at[interval])
        at = early + interval * DMIN

        @pl.loop(0, n, unroll=4)
        def _(b):
            spikes = unpack(inbox[interval, b], rows)
            for offset in range(DMIN):
                history[b * SPAN + at + offset] = spikes[offset * trials : (offset + 1) * trials]

        if interval == 0:
            load.wait()

        def multiply(g, total):
            picked = []
            for j in range(GROUP):
                k = g * GROUP + j
                spot = base_ref[k] + stride_ref[k] * interval
                picked.append(
                    jnp.concatenate([history[spot + s] for s in range(DMIN)], axis=0)
                )
            depth = GROUP * block
            tile = weights_ref[pl.ds(pl.multiple_of(g * depth, depth), depth), :]
            return total + jnp.dot(
                jnp.concatenate(picked, axis=1), tile, preferred_element_type=jnp.float32
            )

        current = lax.fori_loop(
            0, slots // GROUP, multiply, jnp.zeros((pair, block), jnp.float32)
        )
        fired = []
        for offset in range(DMIN):
            arrived = current[offset * trials : (offset + 1) * trials]
            voltage = voltage - jnp.floor(voltage * scale) + arrived + push
            flag = voltage >= THRESHOLD
            voltage = jnp.where(flag, 0.0, jnp.maximum(voltage, -THRESHOLD))
            fired.append(flag)
        if interval < INTERVALS - 1:
            send(interval + 1, pack(jnp.concatenate([f.astype(jnp.int32) for f in fired], axis=0)))
        for offset in range(DMIN):
            ones = jnp.sum(jnp.where(fired[offset], 1.0, 0.0), axis=0, keepdims=True)
            number = jnp.sum(ones, axis=1, keepdims=True)
            counts = jnp.where(count_lane == interval * DMIN + offset, number, counts)

    count_out[...] = counts
    count_in[me] = counts

    @pl.loop(1, n)
    def _(j):
        pltpu.make_async_remote_copy(
            src_ref=count_out,
            dst_ref=count_in.at[me],
            send_sem=send_sem.at[INTERVALS],
            recv_sem=recv_sem.at[INTERVALS],
            device_id=coords(j),
            device_id_type=MESH,
        ).start()

    voltage_ref[...] = voltage
    for interval in range(INTERVALS):
        wait(inbox.at[interval], send_sem.at[interval])
    wait(count_in, send_sem.at[INTERVALS])
    wait(count_in, recv_sem.at[INTERVALS])

    def gather(b, total):
        return total + jnp.where(area_row == area_ref[0, b], count_in[b], 0.0)

    spikes = lax.fori_loop(0, n, gather, jnp.zeros((AREAS, block), jnp.float32), unroll=4)
    rates = spikes / (members * (trials * block))
    rates_ref[...] = jnp.transpose(rates)[0:STEPS]


def solution(mesh):
    sizes = (mesh.shape["area"], mesh.shape["rank"])
    n = sizes[0] * sizes[1]

    def on_device(
        initial_bits, membrane, drive, leak_shift, weights, pre_block, block_mask, delay, area_of_block
    ):
        _, slots, block, width = weights.shape
        trials = membrane.shape[0]
        assert weights.shape[0] == 1 and area_of_block.shape[0] == n
        smem = pl.BlockSpec(memory_space=pltpu.SMEM)
        vmem = pl.BlockSpec(memory_space=pltpu.VMEM)
        return pl.pallas_call(
            functools.partial(kernel, sizes),
            out_shape=(
                jax.ShapeDtypeStruct((trials, block), jnp.float32),
                jax.ShapeDtypeStruct((STEPS, AREAS), jnp.float32),
            ),
            in_specs=[smem] * 4 + [vmem] * 4 + [pl.BlockSpec(memory_space=pl.ANY)],
            out_specs=(vmem, vmem),
            scratch_shapes=[
                pltpu.VMEM((slots * block, width), jnp.bfloat16),
                pltpu.VMEM((n * SPAN, trials, block), jnp.bfloat16),
                pltpu.VMEM((INTERVALS, 4, block), jnp.int32),
                pltpu.VMEM((INTERVALS, n, 4, block), jnp.int32),
                pltpu.VMEM((1, block), jnp.float32),
                pltpu.VMEM((n, 1, block), jnp.float32),
                pltpu.SMEM((slots,), jnp.int32),
                pltpu.SMEM((slots,), jnp.int32),
                pltpu.SemaphoreType.DMA,
                pltpu.SemaphoreType.DMA((INTERVALS + 1,)),
                pltpu.SemaphoreType.DMA((INTERVALS + 1,)),
            ],
            compiler_params=pltpu.CompilerParams(
                collective_id=0, has_side_effects=True, vmem_limit_bytes=60 * 1024 * 1024
            ),
            name="cortex_window",
        )(
            pre_block,
            block_mask,
            delay,
            area_of_block.reshape(1, -1),
            initial_bits,
            membrane,
            drive.reshape(1, -1),
            leak_shift.reshape(1, -1),
            weights.reshape(slots * block, width),
        )

    both = ("area", "rank")
    in_specs = (
        P(None, None, both),
        P(None, both),
        P(both),
        P(both),
        P(both, None, None, None),
        P(both, None),
        P(both, None),
        P(both, None),
        P(),
    )
    return jax.shard_map(
        on_device, mesh=mesh, in_specs=in_specs, out_specs=(P(None, both), P()), check_vma=False
    )
```

```python
import functools

import jax
import jax.numpy as jnp
from jax import lax
from jax.experimental import pallas as pl
from jax.experimental.pallas import tpu as pltpu
from jax.sharding import PartitionSpec as P

AREAS = 32
DMIN = 2
NDELAY = 4
STEPS = 10
DMAX = DMIN + NDELAY - 1
INTERVALS = STEPS // DMIN
SPAN = STEPS + DMAX - DMIN
THRESHOLD = 200.0
GROUP = 64
MESH = pl.DeviceIdType.MESH


def pack(spikes):
    rows = spikes.shape[0] // 8
    word = spikes[0:8]
    for j in range(1, rows):
        word = word | (spikes[8 * j : 8 * j + 8] << j)
    return word[0:4] | (word[4:8] << rows)


def unpack(word, rows):
    word = jnp.concatenate([word, word >> rows], axis=0)
    parts = [(word & (1 << j)) != 0 for j in range(rows)]
    parts = [jnp.where(p, 1.0, 0.0) for p in parts]
    return jnp.concatenate(parts, axis=0).astype(jnp.bfloat16)


def kernel(
    sizes,
    pre_ref,
    mask_ref,
    delay_ref,
    area_ref,
    bits_ref,
    membrane_ref,
    drive_ref,
    leak_ref,
    weights_hbm,
    voltage_ref,
    rates_ref,
    weights_ref,
    history,
    outbox,
    inbox,
    count_out,
    count_in,
    base_ref,
    stride_ref,
    stage,
    weight_sem,
    send_sem,
    recv_sem,
):
    areas_axis, ranks = sizes
    n = areas_axis * ranks
    me = lax.axis_index("area") * ranks + lax.axis_index("rank")
    trials, block = membrane_ref.shape
    slots = pre_ref.shape[1]
    pair = DMIN * trials
    rows = pair // 8

    load = pltpu.make_async_copy(weights_hbm, weights_ref, weight_sem)
    load.start()

    def coords(j):
        other = lax.rem(me + j, n)
        return (other // ranks, lax.rem(other, ranks))

    barrier = pltpu.get_barrier_semaphore()

    @pl.loop(1, n)
    def _(j):
        pl.semaphore_signal(barrier, inc=1, device_id=coords(j), device_id_type=MESH)

    lane = lax.broadcasted_iota(jnp.int32, (trials, block), 1)
    start = []
    per = bits_ref.shape[1]
    stage[...] = jnp.zeros_like(stage)
    for offset in range(DMIN):
        stage[offset * per : (offset + 1) * per, 0:trials] = bits_ref[offset]
    turned = jnp.transpose(stage[...])[0:trials]
    for offset in range(DMIN):
        words = turned[:, offset * per : (offset + 1) * per]
        spread = jnp.broadcast_to(words[:, 0:1], (trials, block))
        for w in range(1, block // 32):
            spread = jnp.where(lane // 32 == w, words[:, w : w + 1], spread)
        start.append((spread >> (lane % 32)) & 1)
    word = pack(jnp.concatenate(start, axis=0))

    def send(interval, word):
        outbox[interval] = word
        inbox[interval, me] = word

        @pl.loop(1, n)
        def _(j):
            pltpu.make_async_remote_copy(
                src_ref=outbox.at[interval],
                dst_ref=inbox.at[interval, me],
                send_sem=send_sem.at[interval],
                recv_sem=recv_sem.at[interval],
                device_id=coords(j),
                device_id_type=MESH,
            ).start()

    def wait(box, sem):
        region = box.at[pl.ds(0, n - 1)]
        pltpu.make_async_copy(region, region, sem).wait()

    pl.semaphore_wait(barrier, n - 1)
    send(0, word)

    @pl.loop(0, slots)
    def _(k):
        on = mask_ref[0, k]
        base_ref[k] = on * (pre_ref[0, k] * SPAN + (DMAX - delay_ref[0, k]))
        stride_ref[k] = on * DMIN

    early = DMAX - DMIN
    blank = jnp.zeros((trials, block), jnp.bfloat16)

    @pl.loop(0, n)
    def _(b):
        for s in range(early):
            history[b * SPAN + s] = blank

    scale = 1.0 / jnp.left_shift(jnp.ones_like(leak_ref[...]), leak_ref[...]).astype(jnp.float32)
    push = drive_ref[...].astype(jnp.float32)
    voltage = jnp.floor(membrane_ref[...])
    count_lane = lax.broadcasted_iota(jnp.int32, (1, block), 1)
    counts = jnp.zeros((1, block), jnp.float32)
    area_row = lax.broadcasted_iota(jnp.int32, (AREAS, block), 0)

    def tally(b, total):
        return total + jnp.where(area_row == area_ref[0, b], 1.0, 0.0)

    members = lax.fori_loop(0, n, tally, jnp.zeros((AREAS, block), jnp.float32))

    for interval in range(INTERVALS):
        wait(inbox.at[interval], recv_sem.at[interval])
        at = early + interval * DMIN

        @pl.loop(0, n, unroll=4)
        def _(b):
            spikes = unpack(inbox[interval, b], rows)
            for offset in range(DMIN):
                history[b * SPAN + at + offset] = spikes[offset * trials : (offset + 1) * trials]

        if interval == 0:
            load.wait()

        def multiply(g, total):
            picked = []
            for j in range(GROUP):
                k = g * GROUP + j
                spot = base_ref[k] + stride_ref[k] * interval
                picked.append(
                    jnp.concatenate([history[spot + s] for s in range(DMIN)], axis=0)
                )
            depth = GROUP * block
            tile = weights_ref[pl.ds(pl.multiple_of(g * depth, depth), depth), :]
            return total + jnp.dot(
                jnp.concatenate(picked, axis=1), tile, preferred_element_type=jnp.float32
            )

        current = lax.fori_loop(
            0, slots // GROUP, multiply, jnp.zeros((pair, block), jnp.float32)
        )
        fired = []
        for offset in range(DMIN):
            arrived = current[offset * trials : (offset + 1) * trials]
            voltage = voltage - jnp.floor(voltage * scale) + arrived + push
            flag = voltage >= THRESHOLD
            voltage = jnp.where(flag, 0.0, jnp.maximum(voltage, -THRESHOLD))
            fired.append(flag)
        if interval < INTERVALS - 1:
            send(interval + 1, pack(jnp.concatenate([f.astype(jnp.int32) for f in fired], axis=0)))
        for offset in range(DMIN):
            ones = jnp.sum(jnp.where(fired[offset], 1.0, 0.0), axis=0, keepdims=True)
            number = jnp.sum(ones, axis=1, keepdims=True)
            counts = jnp.where(count_lane == interval * DMIN + offset, number, counts)

    count_out[...] = counts
    count_in[me] = counts

    @pl.loop(1, n)
    def _(j):
        pltpu.make_async_remote_copy(
            src_ref=count_out,
            dst_ref=count_in.at[me],
            send_sem=send_sem.at[INTERVALS],
            recv_sem=recv_sem.at[INTERVALS],
            device_id=coords(j),
            device_id_type=MESH,
        ).start()

    voltage_ref[...] = voltage
    for interval in range(INTERVALS):
        wait(inbox.at[interval], send_sem.at[interval])
    wait(count_in, send_sem.at[INTERVALS])
    wait(count_in, recv_sem.at[INTERVALS])

    def gather(b, total):
        return total + jnp.where(area_row == area_ref[0, b], count_in[b], 0.0)

    spikes = lax.fori_loop(0, n, gather, jnp.zeros((AREAS, block), jnp.float32), unroll=4)
    rates = spikes / (members * (trials * block))
    rates_ref[...] = jnp.transpose(rates)[0:STEPS]


def hand_over(voltage_in, rates_in, voltage_ref, rates_ref):
    voltage_ref[...] = voltage_in[...]
    rates_ref[...] = rates_in[...]


def solution(mesh):
    sizes = (mesh.shape["area"], mesh.shape["rank"])
    n = sizes[0] * sizes[1]

    def on_device(
        initial_bits, membrane, drive, leak_shift, weights, pre_block, block_mask, delay, area_of_block
    ):
        _, slots, block, width = weights.shape
        trials = membrane.shape[0]
        assert weights.shape[0] == 1 and area_of_block.shape[0] == n
        smem = pl.BlockSpec(memory_space=pltpu.SMEM)
        vmem = pl.BlockSpec(memory_space=pltpu.VMEM)
        voltage, rates = pl.pallas_call(
            functools.partial(kernel, sizes),
            out_shape=(
                jax.ShapeDtypeStruct((trials, block), jnp.float32),
                jax.ShapeDtypeStruct((STEPS, AREAS), jnp.float32),
            ),
            in_specs=[smem] * 4 + [vmem] * 4 + [pl.BlockSpec(memory_space=pl.ANY)],
            out_specs=(vmem, vmem),
            scratch_shapes=[
                pltpu.VMEM((slots * block, width), jnp.bfloat16),
                pltpu.VMEM((n * SPAN, trials, block), jnp.bfloat16),
                pltpu.VMEM((INTERVALS, 4, block), jnp.int32),
                pltpu.VMEM((INTERVALS, n, 4, block), jnp.int32),
                pltpu.VMEM((1, block), jnp.float32),
                pltpu.VMEM((n, 1, block), jnp.float32),
                pltpu.SMEM((slots,), jnp.int32),
                pltpu.SMEM((slots,), jnp.int32),
                pltpu.VMEM((DMIN * (block // 32), block), jnp.int32),
                pltpu.SemaphoreType.DMA,
                pltpu.SemaphoreType.DMA((INTERVALS + 1,)),
                pltpu.SemaphoreType.DMA((INTERVALS + 1,)),
            ],
            compiler_params=pltpu.CompilerParams(
                collective_id=0, has_side_effects=True, vmem_limit_bytes=60 * 1024 * 1024
            ),
            name="cortex_window",
        )(
            pre_block,
            block_mask,
            delay,
            area_of_block.reshape(1, -1),
            initial_bits.transpose(0, 2, 1),
            membrane,
            drive.reshape(1, -1),
            leak_shift.reshape(1, -1),
            weights.reshape(slots * block, width),
        )
        return pl.pallas_call(
            hand_over,
            out_shape=(
                jax.ShapeDtypeStruct(voltage.shape, voltage.dtype),
                jax.ShapeDtypeStruct(rates.shape, rates.dtype),
            ),
            in_specs=[vmem] * 2,
            out_specs=(vmem, vmem),
            name="hand_over",
        )(voltage, rates)

    both = ("area", "rank")
    in_specs = (
        P(None, None, both),
        P(None, both),
        P(both),
        P(both),
        P(both, None, None, None),
        P(both, None),
        P(both, None),
        P(both, None),
        P(),
    )
    return jax.shard_map(
        on_device, mesh=mesh, in_specs=in_specs, out_specs=(P(None, both), P()), check_vma=False
    )
```
